32 devices in a mesh: owner: 4 (over y, core), rows: 8 (over z, x).
Axes of the slice: x: 2, y: 2, z: 4, core: 2. Of those that a mesh axis runs over, the one named last changes fastest.
Arguments:
- train_gate: float32 [128, 2048, 768], P('owner', 'rows'), may hold values from -0.125 to 0.125
- train_up: float32 [128, 2048, 768], P('owner', 'rows'), may hold values from -0.125 to 0.125
- router_weight: float32 [2048, 128], P('rows', 'owner'), may hold values from -0.125 to 0.125
- router_gain: float32 [2048], P('rows'), may hold values from 0.25 to 1.75
Outputs:
- ready_gate: bfloat16 [128, 768, 2048], P(('owner', 'rows'))
- ready_up: bfloat16 [128, 768, 2048], P(('owner', 'rows'))
- serve_router: bfloat16 [2048, 128], replicated
The draws below stay inside these ranges and needn't reach their ends.
All inputs are finite; a program needn't handle non-finite values.
Results may differ from the reference program's by a relative error of at most 0.001.
Values may be sent and summed in bfloat16 or wider, within the bound.
A program may use at most 192 MiB of HBM per device.

```python
import jax
import jax.numpy as jnp

EXPERTS = 128
D_MODEL = 2048
D_EXPERT = 768


def level_of(stream_key, extent, pieces, smallest, top_value):
    level, own = 1.0, jax.random.fold_in(stream_key, 6)
    for position, parts in pieces:
        draws = jnp.exp(jax.random.uniform(jax.random.fold_in(own, position), (parts,), jnp.float32, smallest / len(pieces), top_value / len(pieces)))
        level = level * jnp.repeat(draws, extent[position] // parts).reshape([-1 if axis == position else 1 for axis in range(len(extent))])
    return level


def normal_values(key, shape, deviation, limit, cuts=(), held_as=jnp.bfloat16):
    entries = deviation * jax.random.normal(key, shape, jnp.float32)
    if cuts:
        entries = entries * level_of(key, shape, cuts, -0.22, 0.18)
    return jnp.clip(entries, -limit, limit).astype(held_as)


def setup_inputs(seed: int = 0) -> dict:
    arg_keys = jax.random.split(jax.random.key(seed), 5)
    return {
        "train_gate": normal_values(arg_keys[0], (EXPERTS, D_MODEL, D_EXPERT), D_MODEL ** -0.5, 0.125, ((0, 4), (1, 8)), jnp.float32),
        "train_up": normal_values(arg_keys[1], (EXPERTS, D_MODEL, D_EXPERT), D_MODEL ** -0.5, 0.125, ((0, 4), (1, 8)), jnp.float32),
        "router_weight": normal_values(arg_keys[2], (D_MODEL, EXPERTS), D_MODEL ** -0.5, 0.125, ((0, 8), (1, 4)), jnp.float32),
        "router_gain": jnp.clip(1.0 + 0.15 * jax.random.normal(arg_keys[3], (D_MODEL,), jnp.float32), 0.25, 1.75),
    }


def reference(train_gate, train_up, router_weight, router_gain):
    ready_gate = train_gate.astype(jnp.bfloat16)
    ready_gate = jnp.transpose(ready_gate, (0, 2, 1))
    ready_up = train_up.astype(jnp.bfloat16)
    ready_up = jnp.transpose(ready_up, (0, 2, 1))
    serve_router = (router_weight * router_gain[:, None]).astype(jnp.bfloat16)
    return ready_gate, ready_up, serve_router
```

```python
import functools

import jax
import jax.numpy as jnp
from jax import lax
from jax.experimental import pallas as pl
from jax.experimental.pallas import tpu as pltpu
from jax.sharding import PartitionSpec as P

STAGES = 4
LANES = 128


def targets_of(n):
    half, quarter = n // 2, max(n // 4, 1)
    table = []
    for r in range(n):
        others = [t for t in range(n) if t != r]
        near = [t for t in others if (t < half) == (r < half)]
        far = [t for t in others if t not in near]
        outer = r // quarter in (0, (n - 1) // quarter)
        if outer:
            order = near + far
        else:
            order = []
            near, far = list(near), list(far)
            while near or far:
                order += far[:1] + near[:1]
                near, far = near[1:], far[1:]
        table.append((order, outer))
    return table


def pick(values, index):
    result = jnp.int32(values[0])
    for place, value in enumerate(values[1:], 1):
        result = jnp.where(index == place, jnp.int32(value), result)
    return result


def kernel(
    n, owners, gate, up, router, gain, out_gate, out_up, out_router,
    stage, sent, row_router, stage_sem, send_sem, recv_sem,
    row_send, row_recv, owner_send, owner_recv,
):
    me = lax.axis_index("rows")
    my_owner = lax.axis_index("owner")
    width, each = gate.shape[1], gate.shape[0] // n
    wide = router.shape[0]
    chunks = 2 * each
    remote = (n - 1) * chunks
    total = n * chunks
    table = targets_of(n)
    outer = pick([int(o) for _, o in table], me) == 1

    def place(step):
        by_target = step // chunks
        order = jnp.where(outer, by_target, step % (n - 1))
        chunk = jnp.where(outer, step % chunks, step // (n - 1))
        target = jnp.int32(0)
        for s in range(n - 1):
            target = jnp.where(order == s, pick([o[s] for o, _ in table], me), target)
        own = step >= remote
        target = jnp.where(own, me, target)
        chunk = jnp.where(own, step - remote, chunk)
        return target, chunk

    def load(step):
        target, chunk = place(step)
        slot = step % STAGES
        for index, source in enumerate((gate, up)):

            @pl.when(chunk // each == index)
            def _():
                pltpu.make_async_copy(
                    source.at[target * each + chunk % each], stage.at[slot], stage_sem.at[slot]
                ).start()

    def narrow(slot):
        pltpu.make_async_copy(gate.at[0], stage.at[slot], stage_sem.at[slot]).wait()
        return stage[slot].astype(jnp.bfloat16).T

    for step in range(STAGES):
        load(jnp.int32(step))

    barrier = pltpu.get_barrier_semaphore()
    for d in range(1, n):
        pl.semaphore_signal(barrier, inc=1, device_id={"rows": lax.rem(me + d, n)})
    for d in range(1, owners):
        pl.semaphore_signal(barrier, inc=1, device_id={"owner": lax.rem(my_owner + d, owners)})
    pl.semaphore_wait(barrier, n - 1 + owners - 1)

    columns = pl.ds(pl.multiple_of(me * width, width), width)

    def remote_step(step, carry):
        target, chunk = place(step)
        slot = step % STAGES
        sent[step] = narrow(slot)
        load(step + STAGES)
        for index, out in enumerate((out_gate, out_up)):

            @pl.when(chunk // each == index)
            def _():
                pltpu.make_async_remote_copy(
                    src_ref=sent.at[step],
                    dst_ref=out.at[chunk % each, :, columns],
                    send_sem=send_sem.at[step],
                    recv_sem=recv_sem.at[me * chunks + chunk],
                    device_id={"rows": target},
                ).start()

        return carry

    lax.fori_loop(0, 1, remote_step, 0)

    row_router[:, columns] = (router[...] * gain[...]).astype(jnp.bfloat16)

    def row_copy(d, source):
        span = pl.ds(pl.multiple_of(source * width, width), width)
        return pltpu.make_async_remote_copy(
            src_ref=row_router.at[:, span],
            dst_ref=row_router.at[:, span],
            send_sem=row_send.at[d],
            recv_sem=row_recv.at[d],
            device_id={"rows": lax.rem(me + d, n)},
        )

    for d in range(1, n):
        row_copy(d, me).start()

    lax.fori_loop(1, remote, remote_step, 0)

    def own_step(step, carry):
        chunk = step - remote
        mine = narrow(step % STAGES)

        @pl.when(step + STAGES < total)
        def _():
            load(step + STAGES)

        for index, out in enumerate((out_gate, out_up)):

            @pl.when(chunk // each == index)
            def _():
                out[chunk % each, :, columns] = mine

        return carry

    lax.fori_loop(remote, total, own_step, 0)

    for d in range(1, n):
        row_copy(d, lax.rem(me + n - d, n)).wait_recv()
        row_copy(d, me).wait_send()
    owned = pl.ds(pl.multiple_of(my_owner * wide, wide), wide)
    out_router[owned, :] = row_router[...]
    owner_copies = [
        pltpu.make_async_remote_copy(
            src_ref=row_router,
            dst_ref=out_router.at[owned, :],
            send_sem=owner_send.at[d],
            recv_sem=owner_recv.at[d],
            device_id={"owner": lax.rem(my_owner + d, owners)},
        )
        for d in range(1, owners)
    ]
    for copy in owner_copies:
        copy.start()
    for copy in owner_copies:
        copy.wait()

    def chunk_copy(send, recv):
        return pltpu.make_async_remote_copy(
            src_ref=sent.at[0],
            dst_ref=out_gate.at[0, :, columns],
            send_sem=send_sem.at[send],
            recv_sem=recv_sem.at[recv],
            device_id={"rows": lax.rem(me + 1, n)},
        )

    def drain(step, carry):
        source = lax.rem(me + 1 + step // chunks, n)
        chunk_copy(step, source * chunks + step % chunks).wait_recv()
        chunk_copy(step, 0).wait_send()
        return carry

    lax.fori_loop(0, remote, drain, 0)


def exchange(n, owners, train_gate, train_up, router_weight, router_gain):
    experts, width, inner = train_gate.shape
    each, wide = experts // n, router_weight.shape[1]
    chunks = 2 * each
    ready = pltpu.VMEM((each, inner, n * width), jnp.bfloat16)
    dma = pltpu.SemaphoreType.DMA
    vmem = pl.BlockSpec(memory_space=pltpu.VMEM)
    hbm = pl.BlockSpec(memory_space=pl.ANY)
    ready_gate, ready_up, router = pl.pallas_call(
        functools.partial(kernel, n, owners),
        out_shape=(ready, ready, pltpu.VMEM((owners * wide, n * width), jnp.bfloat16)),
        in_specs=[hbm, hbm, vmem, vmem],
        out_specs=(vmem, vmem, vmem),
        scratch_shapes=[
            pltpu.VMEM((STAGES, width, inner), jnp.float32),
            pltpu.VMEM(((n - 1) * chunks, inner, width), jnp.bfloat16),
            pltpu.VMEM((wide, n * width), jnp.bfloat16),
            dma((STAGES,)),
            dma(((n - 1) * chunks,)),
            dma((n * chunks,)),
            dma((n,)),
            dma((n,)),
            dma((owners,)),
            dma((owners,)),
        ],
        compiler_params=pltpu.CompilerParams(
            collective_id=0, has_side_effects=True, vmem_limit_bytes=KERNEL_VMEM
        ),
    )(train_gate, train_up, router_weight.T, router_gain[None, :])
    ready_gate, ready_up = put_out(ready_gate, ready_up)
    return ready_gate, ready_up, router.T


def put_out(*arrays):
    def body(*refs):
        sources, outs, sem = refs[: len(arrays)], refs[len(arrays) : -1], refs[-1]
        copies = [
            pltpu.make_async_copy(source.at[part], out.at[part], sem.at[index, part])
            for index, (source, out) in enumerate(zip(sources, outs))
            for part in range(source.shape[0])
        ]
        for copy in copies:
            copy.start()
        for copy in copies:
            copy.wait()

    return pl.pallas_call(
        body,
        out_shape=[jax.ShapeDtypeStruct(a.shape, a.dtype) for a in arrays],
        in_specs=[pl.BlockSpec(memory_space=pltpu.VMEM)] * len(arrays),
        out_specs=[pl.BlockSpec(memory_space=pl.ANY)] * len(arrays),
        scratch_shapes=[pltpu.SemaphoreType.DMA((len(arrays), arrays[0].shape[0]))],
        compiler_params=pltpu.CompilerParams(vmem_limit_bytes=1024 * 1024),
    )(*[pltpu.with_memory_space_constraint(a, pltpu.VMEM) for a in arrays])


KERNEL_VMEM = 32 * 1024 * 1024


def plain(train_gate, train_up, router_weight, router_gain):
    narrow_gate, narrow_up = (train_gate.astype(jnp.bfloat16), train_up.astype(jnp.bfloat16))
    ready_gate, ready_up = (
        lax.all_to_all(narrow_gate, "rows", split_axis=0, concat_axis=1, tiled=True),
        lax.all_to_all(narrow_up, "rows", split_axis=0, concat_axis=1, tiled=True),
    )
    ready_gate = jnp.transpose(ready_gate, (0, 2, 1))
    ready_up = jnp.transpose(ready_up, (0, 2, 1))
    part_router = (router_weight * router_gain[:, None]).astype(jnp.bfloat16)
    row_router = lax.all_gather(part_router, "rows", axis=0, tiled=True)
    serve_router = lax.all_gather(row_router, "owner", axis=1, tiled=True)
    return ready_gate, ready_up, serve_router


def solution(mesh):
    n, owners = mesh.shape["rows"], mesh.shape["owner"]

    def on_device(train_gate, train_up, router_weight, router_gain):
        if n > 1 and owners > 1 and train_gate.shape[1] % LANES == 0 and router_weight.shape[1] % 16 == 0:
            return exchange(n, owners, train_gate, train_up, router_weight, router_gain)
        return plain(train_gate, train_up, router_weight, router_gain)

    placed = (P("owner", "rows", None), P("owner", "rows", None), P("rows", "owner"), P("rows"))
    return jax.shard_map(
        on_device,
        mesh=mesh,
        in_specs=placed,
        out_specs=(P(("owner", "rows"), None, None), P(("owner", "rows"), None, None), P()),
        check_vma=False,
    )
```

```python
import functools

import jax
import jax.numpy as jnp
from jax import lax
from jax.experimental import pallas as pl
from jax.experimental.pallas import tpu as pltpu
from jax.sharding import PartitionSpec as P

STAGES = 4
LANES = 128


def targets_of(n):
    half, quarter = n // 2, max(n // 4, 1)
    table = []
    for r in range(n):
        others = sorted(
            (t for t in range(n) if t != r),
            key=lambda t: (-abs(t // quarter - r // quarter), -((t - r) % quarter)),
        )
        near = [t for t in others if (t < half) == (r < half)]
        far = [t for t in others if t not in near]
        outer = r // quarter in (0, (n - 1) // quarter)
        if outer:
            order = near + far
        else:
            order = []
            near, far = list(near), list(far)
            while near or far:
                order += far[:1] + near[:1]
                near, far = near[1:], far[1:]
        table.append((order, outer))
    return table


def pick(values, index):
    result = jnp.int32(values[0])
    for place, value in enumerate(values[1:], 1):
        result = jnp.where(index == place, jnp.int32(value), result)
    return result


def kernel(
    n, owners, gate, up, router, gain, out_gate, out_up, out_router,
    stage, sent, row_router, stage_sem, send_sem, recv_sem,
    row_send, row_recv, owner_send, owner_recv,
):
    me = lax.axis_index("rows")
    my_owner = lax.axis_index("owner")
    width, each = gate.shape[1], gate.shape[0] // n
    wide = router.shape[0]
    chunks = 2 * each
    remote = (n - 1) * chunks
    total = n * chunks
    table = targets_of(n)
    outer = pick([int(o) for _, o in table], me) == 1

    def place(step):
        by_target = step // chunks
        order = jnp.where(outer, by_target, step % (n - 1))
        chunk = jnp.where(outer, step % chunks, step // (n - 1))
        target = jnp.int32(0)
        for s in range(n - 1):
            target = jnp.where(order == s, pick([o[s] for o, _ in table], me), target)
        own = step >= remote
        target = jnp.where(own, me, target)
        chunk = jnp.where(own, step - remote, chunk)
        return target, chunk

    def load(step):
        target, chunk = place(step)
        slot = step % STAGES
        for index, source in enumerate((gate, up)):

            @pl.when(chunk // each == index)
            def _():
                pltpu.make_async_copy(
                    source.at[target * each + chunk % each], stage.at[slot], stage_sem.at[slot]
                ).start()

    def narrow(slot):
        pltpu.make_async_copy(gate.at[0], stage.at[slot], stage_sem.at[slot]).wait()
        return stage[slot].astype(jnp.bfloat16).T

    for step in range(STAGES):
        load(jnp.int32(step))

    barrier = pltpu.get_barrier_semaphore()
    for d in range(1, n):
        pl.semaphore_signal(barrier, inc=1, device_id={"rows": lax.rem(me + d, n)})
    for d in range(1, owners):
        pl.semaphore_signal(barrier, inc=1, device_id={"owner": lax.rem(my_owner + d, owners)})
    pl.semaphore_wait(barrier, n - 1 + owners - 1)

    columns = pl.ds(pl.multiple_of(me * width, width), width)

    def remote_step(step, carry):
        target, chunk = place(step)
        slot = step % STAGES
        sent[step] = narrow(slot)
        load(step + STAGES)
        for index, out in enumerate((out_gate, out_up)):

            @pl.when(chunk // each == index)
            def _():
                pltpu.make_async_remote_copy(
                    src_ref=sent.at[step],
                    dst_ref=out.at[chunk % each, :, columns],
                    send_sem=send_sem.at[step],
                    recv_sem=recv_sem.at[me * chunks + chunk],
                    device_id={"rows": target},
                ).start()

        return carry

    lax.fori_loop(0, 1, remote_step, 0)

    row_router[:, columns] = (router[...] * gain[...]).astype(jnp.bfloat16)

    def row_copy(d, source):
        span = pl.ds(pl.multiple_of(source * width, width), width)
        return pltpu.make_async_remote_copy(
            src_ref=row_router.at[:, span],
            dst_ref=row_router.at[:, span],
            send_sem=row_send.at[d],
            recv_sem=row_recv.at[d],
            device_id={"rows": lax.rem(me + d, n)},
        )

    for d in range(1, n):
        row_copy(d, me).start()

    lax.fori_loop(1, remote, remote_step, 0)

    def own_step(step, carry):
        chunk = step - remote
        mine = narrow(step % STAGES)

        @pl.when(step + STAGES < total)
        def _():
            load(step + STAGES)

        for index, out in enumerate((out_gate, out_up)):

            @pl.when(chunk // each == index)
            def _():
                out[chunk % each, :, columns] = mine

        return carry

    lax.fori_loop(remote, total, own_step, 0)

    for d in range(1, n):
        row_copy(d, lax.rem(me + n - d, n)).wait_recv()
        row_copy(d, me).wait_send()
    owned = pl.ds(pl.multiple_of(my_owner * wide, wide), wide)
    out_router[owned, :] = row_router[...]
    owner_copies = [
        pltpu.make_async_remote_copy(
            src_ref=row_router,
            dst_ref=out_router.at[owned, :],
            send_sem=owner_send.at[d],
            recv_sem=owner_recv.at[d],
            device_id={"owner": lax.rem(my_owner + d, owners)},
        )
        for d in range(1, owners)
    ]
    for copy in owner_copies:
        copy.start()
    for copy in owner_copies:
        copy.wait()

    def chunk_copy(send, recv):
        return pltpu.make_async_remote_copy(
            src_ref=sent.at[0],
            dst_ref=out_gate.at[0, :, columns],
            send_sem=send_sem.at[send],
            recv_sem=recv_sem.at[recv],
            device_id={"rows": lax.rem(me + 1, n)},
        )

    def drain(step, carry):
        source = lax.rem(me + 1 + step // chunks, n)
        chunk_copy(step, source * chunks + step % chunks).wait_recv()
        chunk_copy(step, 0).wait_send()
        return carry

    lax.fori_loop(0, remote, drain, 0)


def exchange(n, owners, train_gate, train_up, router_weight, router_gain):
    experts, width, inner = train_gate.shape
    each, wide = experts // n, router_weight.shape[1]
    chunks = 2 * each
    ready = pltpu.VMEM((each, inner, n * width), jnp.bfloat16)
    dma = pltpu.SemaphoreType.DMA
    vmem = pl.BlockSpec(memory_space=pltpu.VMEM)
    hbm = pl.BlockSpec(memory_space=pl.ANY)
    ready_gate, ready_up, router = pl.pallas_call(
        functools.partial(kernel, n, owners),
        out_shape=(ready, ready, pltpu.VMEM((owners * wide, n * width), jnp.bfloat16)),
        in_specs=[hbm, hbm, vmem, vmem],
        out_specs=(vmem, vmem, vmem),
        scratch_shapes=[
            pltpu.VMEM((STAGES, width, inner), jnp.float32),
            pltpu.VMEM(((n - 1) * chunks, inner, width), jnp.bfloat16),
            pltpu.VMEM((wide, n * width), jnp.bfloat16),
            dma((STAGES,)),
            dma(((n - 1) * chunks,)),
            dma((n * chunks,)),
            dma((n,)),
            dma((n,)),
            dma((owners,)),
            dma((owners,)),
        ],
        compiler_params=pltpu.CompilerParams(
            collective_id=0, has_side_effects=True, vmem_limit_bytes=KERNEL_VMEM
        ),
    )(train_gate, train_up, router_weight.T, router_gain[None, :])
    ready_gate, ready_up = put_out(ready_gate, ready_up)
    return ready_gate, ready_up, router.T


def put_out(*arrays):
    def body(*refs):
        sources, outs, sem = refs[: len(arrays)], refs[len(arrays) : -1], refs[-1]
        copies = [
            pltpu.make_async_copy(source.at[part], out.at[part], sem.at[index, part])
            for index, (source, out) in enumerate(zip(sources, outs))
            for part in range(source.shape[0])
        ]
        for copy in copies:
            copy.start()
        for copy in copies:
            copy.wait()

    return pl.pallas_call(
        body,
        out_shape=[jax.ShapeDtypeStruct(a.shape, a.dtype) for a in arrays],
        in_specs=[pl.BlockSpec(memory_space=pltpu.VMEM)] * len(arrays),
        out_specs=[pl.BlockSpec(memory_space=pl.ANY)] * len(arrays),
        scratch_shapes=[pltpu.SemaphoreType.DMA((len(arrays), arrays[0].shape[0]))],
        compiler_params=pltpu.CompilerParams(vmem_limit_bytes=1024 * 1024),
    )(*[pltpu.with_memory_space_constraint(a, pltpu.VMEM) for a in arrays])


KERNEL_VMEM = 32 * 1024 * 1024


def plain(train_gate, train_up, router_weight, router_gain):
    narrow_gate, narrow_up = (train_gate.astype(jnp.bfloat16), train_up.astype(jnp.bfloat16))
    ready_gate, ready_up = (
        lax.all_to_all(narrow_gate, "rows", split_axis=0, concat_axis=1, tiled=True),
        lax.all_to_all(narrow_up, "rows", split_axis=0, concat_axis=1, tiled=True),
    )
    ready_gate = jnp.transpose(ready_gate, (0, 2, 1))
    ready_up = jnp.transpose(ready_up, (0, 2, 1))
    part_router = (router_weight * router_gain[:, None]).astype(jnp.bfloat16)
    row_router = lax.all_gather(part_router, "rows", axis=0, tiled=True)
    serve_router = lax.all_gather(row_router, "owner", axis=1, tiled=True)
    return ready_gate, ready_up, serve_router


def solution(mesh):
    n, owners = mesh.shape["rows"], mesh.shape["owner"]

    def on_device(train_gate, train_up, router_weight, router_gain):
        if n > 1 and owners > 1 and train_gate.shape[1] % LANES == 0 and router_weight.shape[1] % 16 == 0:
            return exchange(n, owners, train_gate, train_up, router_weight, router_gain)
        return plain(train_gate, train_up, router_weight, router_gain)

    placed = (P("owner", "rows", None), P("owner", "rows", None), P("rows", "owner"), P("rows"))
    return jax.shard_map(
        on_device,
        mesh=mesh,
        in_specs=placed,
        out_specs=(P(("owner", "rows"), None, None), P(("owner", "rows"), None, None), P()),
        check_vma=False,
    )
```
